256 devices in a mesh: freq: 2 (over core), row: 8 (over y_hi, x), col: 16 (over z, y_lo).
Axes of the slice: x: 4, y: 4 (y_hi: 2, y_lo: 2; y = y_hi * 2 + y_lo), z: 8, core: 2. Of those that a mesh axis runs over, the one named last changes fastest.
Arguments:
- coupling: bfloat16 [12288, 6144], P('row', 'col'), may hold values from -0.109375 to 0.109375
- freq_weight: float32 [24576], P(('freq', 'row')), parts along dimension 0, may hold values from 0.05 to 2
Outputs:
- response: float32 [12288, 6144], P(('freq', 'row'), 'col'), parts along dimension 0
The draws below stay inside these ranges and needn't reach their ends.
There are 2 independent parts, one for each index of `freq`. The reference program is written for one: setup_inputs(seed, part) draws one part's arguments, and reference() takes and returns one part's arrays. A program takes and returns all parts, laid end to end along the dimension named above; an argument that names none is the same for every part. Nothing has to cross between parts.
All inputs are finite; a program needn't handle non-finite values.
Results may differ from the reference program's by a relative error of at most 0.0021.
Values may be sent and summed in bfloat16 or wider, within the bound.
No kernel may reach another device: no remote copies, remote signals or barrier semaphores. Data moves between devices by JAX's collectives and lax.ppermute only.
A program may use at most 128 MiB of HBM per device.

```python
import jax
import jax.numpy as jnp
from jax import lax

NAUX = 6144
NV = 12288


def draw_freq_weight(key, part):
    key_level = jax.random.fold_in(key, 11)
    key_floor = jax.random.fold_in(key, 23)
    level = jax.random.uniform(key_level, (NV,), jnp.float32)
    values = 0.05 * jnp.exp(level * jnp.log(40.0))
    at_floor = jax.random.uniform(key_floor, (NV,), jnp.float32) < 0.1
    values = jnp.where(at_floor, jnp.float32(0.05), values)
    return jnp.clip(values, 0.05, 2.0).astype(jnp.float32)


def block_levels(own_key, extent, shards, least, high):
    loudness, own = 1.0, jax.random.fold_in(own_key, 6)
    for position, parts in shards:
        draws = jnp.exp(jax.random.uniform(jax.random.fold_in(own, position), (parts,), jnp.float32, least / len(shards), high / len(shards)))
        loudness = loudness * jnp.repeat(draws, extent[position] // parts).reshape([-1 if axis == position else 1 for axis in range(len(extent))])
    return loudness


def centred(key, shape, spread, most, split=(), dtype=jnp.bfloat16):
    array = spread * jax.random.normal(key, shape, jnp.float32)
    if split:
        array = array * block_levels(key, shape, split, -0.22, 0.18)
    return jnp.clip(array, -most, most).astype(dtype)


def setup_inputs(seed: int = 0, part: int = 0) -> dict:
    splits = jax.random.split(jax.random.key(seed), 3)
    own_keys = jax.random.split(jax.random.fold_in(splits[2], part), 3)
    return {
        "coupling": centred(splits[0], (NV, NAUX), (NV // 4) ** -0.5, 0.109375, ((0, 8), (1, 16))),
        "freq_weight": draw_freq_weight(jax.random.fold_in(jax.random.fold_in(splits[2], part), 71), part),
    }


def reference(coupling, freq_weight):
    weighted = (coupling.astype(jnp.float32) * freq_weight[:, None]).astype(jnp.bfloat16)
    return jnp.dot(weighted.astype(jnp.float32).T, coupling.astype(jnp.float32),
                   precision=lax.Precision.HIGHEST, preferred_element_type=jnp.float32)
```

```python
import jax
import jax.numpy as jnp
from jax import lax
from jax.sharding import Mesh
from jax.sharding import PartitionSpec as P

FREQ, YH, X, Z, YL = 2, 2, 4, 8, 2
AXES = ("f", "yh", "x", "z", "yl")
CHUNKS = 3


def place(f, yh, x, z, yl):
    return (((f * YH + yh) * X + x) * Z + z) * YL + yl


def ring_pairs(size, sign, cores=(0, 1)):
    pairs = []
    for f in cores:
        step = sign if f == 0 else -sign
        pairs += [(f * size + i, f * size + (i + step) % size) for i in range(size)]
    return pairs


def home_yh(f, x, z, late):
    j = (z - x) % X if f == 0 else (x - z) % X
    if j == 0 and f == late:
        j = X
    r = (z - j if f == 0 else z + j) % Z
    return r // X


def y_pairs(k1, k0, late):
    pairs = []
    for f in range(FREQ):
        for yh in range(YH):
            for x in range(X):
                for z in range(Z):
                    for yl in range(YL):
                        there = place(yh ^ k1, home_yh(f, x, z, late), x, z, yl ^ k0)
                        pairs.append((place(f, yh, x, z, yl), there))
    return pairs


def on_device(coupling, freq_weight):
    f, yh, x, z, yl = (lax.axis_index(a) for a in AXES)
    rows, cols = coupling.shape
    width = cols // CHUNKS
    other_weight = lax.ppermute(freq_weight, "f", [(0, 1), (1, 0)])
    weight = [
        jnp.where(f == 0, freq_weight, other_weight)[:, None],
        jnp.where(f == 0, other_weight, freq_weight)[:, None],
    ]
    beside = lax.ppermute(coupling, "yl", [(0, 1), (1, 0)])
    right = jnp.concatenate([coupling, beside], axis=1)
    first = jnp.where(f == 0, z - x, x - z) % X
    blocks = []
    for c in range(CHUNKS):
        late = 1 - c % 2
        own = coupling[:, c * width : (c + 1) * width]
        held = [own]
        for step in range(4):
            cores = (0, 1) if step < 3 else (late,)
            held.append(lax.ppermute(held[-1], ("f", "z"), ring_pairs(Z, 1, cores)))
        slots = [jnp.where(f == late, held[4], own)] + held[1:4]

        def product(delta):
            at = (first - delta) % X
            tile = jnp.where(
                at < 2,
                jnp.where(at == 0, slots[0], slots[1]),
                jnp.where(at == 2, slots[2], slots[3]),
            ).astype(jnp.float32)
            left = jnp.concatenate(
                [(tile * w).astype(jnp.bfloat16) for w in weight], axis=1
            )
            return lax.dot_general(
                left, right, (((0,), (0,)), ((), ())), preferred_element_type=jnp.float32
            )

        relay = lax.ppermute(product(2).astype(jnp.bfloat16), ("f", "x"), ring_pairs(X, 1))
        back = lax.ppermute(product(3).astype(jnp.bfloat16), ("f", "x"), ring_pairs(X, -1))
        ahead = (product(1) + relay.astype(jnp.float32)).astype(jnp.bfloat16)
        ahead = lax.ppermute(ahead, ("f", "x"), ring_pairs(X, 1))
        total = product(0) + back.astype(jnp.float32) + ahead.astype(jnp.float32)
        total = total.astype(jnp.bfloat16).reshape(FREQ, width, YL, cols)
        halves = []
        for k0 in range(YL):
            parts = []
            for k1 in range(YH):
                piece = jnp.where(yh == k1, total[0, :, k0], total[1, :, k0])
                parts.append(lax.ppermute(piece, AXES, y_pairs(k1, k0, late)))
            halves.append(parts[0].astype(jnp.float32) + parts[1].astype(jnp.float32))
        blocks.append(halves)
    even = [jnp.where(yl == 0, h[0], h[1]) for h in blocks]
    odd = [jnp.where(yl == 0, h[1], h[0]) for h in blocks]
    return jnp.concatenate(even + odd, axis=0)


def solution(mesh):
    torus = Mesh(mesh.devices.reshape(FREQ, YH, X, Z, YL), AXES)
    placed = (P(("yh", "x"), ("z", "yl")), P(("f", "yh", "x")))
    return jax.shard_map(
        on_device,
        mesh=torus,
        in_specs=placed,
        out_specs=P(("f", "yh", "x"), ("z", "yl")),
        check_vma=False,
    )
```

```python
import functools

import jax
import jax.numpy as jnp
import numpy as np
from jax import lax
from jax.experimental import pallas as pl
from jax.experimental.pallas import tpu as pltpu
from jax.sharding import Mesh
from jax.sharding import PartitionSpec as P


FREQ, YH, X, Z, YL = 2, 2, 4, 8, 2
AXES = ("f", "yh", "x", "z", "yl")
CHUNKS = 3
GROUPS = ((0,), (1, 2))
SWAP = [(0, 1), (1, 0)]


FACTS, PER_CHUNK = 3, 5


def late_core(c):
    return 1 - c % 2


def lookup_table():
    rows = []
    for f, yh, x, z, yl in np.ndindex(FREQ, YH, X, Z, YL):
        row = [f, yh, yl]
        first = (z - x if f == 0 else x - z) % X
        for c in range(CHUNKS):
            at = [(first - delta) % X for delta in range(X)]
            at = [X if j == 0 and f == late_core(c) else j for j in at]
            home = ((z - at[0] if f == 0 else z + at[0]) % Z) // X
            row += at + [home]
        rows.append(row)
    return np.array(rows, np.int32)


def ring_pairs(size, sign, cores=(0, 1)):
    pairs = []
    for f in cores:
        step = sign if f == 0 else -sign
        pairs += [(f * size + i, f * size + (i + step) % size) for i in range(size)]
    return pairs


def kernel_call(kernel, facts, args, out_shape, flops=1 << 28, scratch_shapes=()):
    vmem = pl.BlockSpec(memory_space=pltpu.VMEM)
    return pl.pallas_call(
        kernel,
        out_shape=out_shape,
        in_specs=[pl.BlockSpec(memory_space=pltpu.SMEM)] + [vmem] * len(args),
        out_specs=jax.tree.map(lambda _: vmem, out_shape),
        scratch_shapes=scratch_shapes,
        compiler_params=pltpu.CompilerParams(vmem_limit_bytes=12 << 20),
        cost_estimate=pl.CostEstimate(flops=flops, bytes_accessed=4 << 20, transcendentals=0),
    )(facts, *args)


def half_kernel(facts_ref, tile_ref, out_ref):
    rows = out_ref.shape[0]
    out_ref[...] = tile_ref[pl.ds(pl.multiple_of(facts_ref[0] * rows, rows), rows), :]


def right_kernel(facts_ref, own_ref, part_ref, rest_ref, out_ref):
    rows, cols = part_ref.shape
    for yl in range(YL):
        own_cols = slice(yl * cols, (yl + 1) * cols)
        other_cols = slice((1 - yl) * cols, (2 - yl) * cols)

        @pl.when(facts_ref[2] == yl)
        def _():
            out_ref[:, own_cols] = own_ref[...]
            for f in range(FREQ):
                mine, swapped = (pl.ds(h * rows, rows) for h in (f, 1 - f))

                @pl.when(facts_ref[0] == f)
                def _():
                    out_ref[mine, other_cols] = part_ref[...]
                    out_ref[swapped, other_cols] = rest_ref[...]


def product_kernel(base, facts_ref, *refs):
    tiles, (own_ref, other_ref, right_ref, out_ref, left_ref) = refs[:-5], refs[-5:]
    rows, width = tiles[0].shape
    tall = rows // 6 if rows % 96 == 0 else rows

    @pl.loop(0, out_ref.shape[0])
    def _(k):
        for number, tile_ref in enumerate(tiles):

            @pl.when(facts_ref[base + k] == number)
            def _():
                @pl.loop(0, rows // tall)
                def _(i):
                    part = pl.ds(i * tall, tall)
                    tile = tile_ref[part, :].astype(jnp.float32)
                    for g, weight_ref in enumerate((own_ref, other_ref)):
                        scaled = (tile * weight_ref[part, :]).astype(jnp.bfloat16)
                        left_ref[part, g * width : (g + 1) * width] = scaled

        out_ref[k] = lax.dot_general(
            left_ref[...],
            right_ref[...],
            (((0,), (0,)), ((), ())),
            preferred_element_type=jnp.float32,
        ).astype(out_ref.dtype)


def products(base, facts, tiles, own_weight, other_weight, right, dtype):
    rows, width = tiles[0].shape
    wide = right.shape[1]
    return kernel_call(
        functools.partial(product_kernel, base),
        facts,
        (*tiles, own_weight, other_weight, right),
        jax.ShapeDtypeStruct((2, FREQ * width, wide), dtype),
        4 * FREQ * width * wide * rows,
        (pltpu.VMEM((rows, FREQ * width), jnp.bfloat16),),
    )


def sum_kernel(facts_ref, *refs):
    parts, (mine_ref, away_ref) = refs[:-2], refs[-2:]
    width = mine_ref.shape[1]
    for i in range(mine_ref.shape[0]):
        own_ref, back_ref, ahead_ref = parts[3 * i : 3 * i + 3]
        for half, out_ref in enumerate((mine_ref, away_ref)):
            part = slice(half * width, (half + 1) * width)
            total = own_ref[0, part, :] + back_ref[part, :].astype(jnp.float32)
            out_ref[i] = total + ahead_ref[part, :].astype(jnp.float32)


def arrange_kernel(group, facts_ref, mine_ref, came_ref, kept_ref, *sent):
    width, cols = mine_ref.shape[1], mine_ref.shape[2] // YL
    here = facts_ref[1] * YL + facts_ref[2]
    for i, c in enumerate(group):
        part = pl.ds(i * width, width)
        home = facts_ref[FACTS + PER_CHUNK * c + X]
        for source_ref, away in ((mine_ref, 0), (came_ref, 1)):
            for there in range(YH * YL):
                yh, yl = divmod(there, YL)
                for d in range(YH * YL):

                    @pl.when((home == yh ^ away) & (here == (there - d) % (YH * YL)))
                    def _():
                        block = source_ref[i, :, yl * cols : (yl + 1) * cols]
                        out_ref = sent[d - 1] if d else kept_ref
                        out_ref[part, :] = block.astype(out_ref.dtype)


def final_kernel(groups, facts_ref, *refs):
    out_ref, parts = refs[-1], refs[:-1]
    cols = out_ref.shape[1]
    width = cols // CHUNKS
    for number, group in enumerate(groups):
        kept_ref, one_ref, two_ref, three_ref = parts[4 * number : 4 * number + 4]
        for i, c in enumerate(group):
            part = pl.ds(i * width, width)
            near = kept_ref[part, :] + two_ref[part, :].astype(jnp.float32)
            far = one_ref[part, :].astype(jnp.float32) + three_ref[part, :].astype(jnp.float32)
            for yl in range(YL):

                @pl.when(facts_ref[2] == yl)
                def _():
                    out_ref[pl.ds(yl * cols + c * width, width), :] = near
                    out_ref[pl.ds((1 - yl) * cols + c * width, width), :] = far


def on_device(coupling, freq_weight):
    rows, cols = coupling.shape
    width = cols // CHUNKS
    facts = jnp.asarray(lookup_table())
    facts = lax.dynamic_index_in_dim(facts, lax.axis_index(AXES), keepdims=False)

    half = jax.ShapeDtypeStruct((rows // 2, cols), coupling.dtype)
    part = lax.ppermute(kernel_call(half_kernel, facts, (coupling,), half), "yl", SWAP)
    other_weight = lax.ppermute(freq_weight, "f", SWAP)
    own_weight, other_weight = (
        jnp.broadcast_to(w[:, None], (rows, width)) for w in (freq_weight, other_weight)
    )
    rest = lax.ppermute(part, "f", SWAP)
    both = jax.ShapeDtypeStruct((rows, YL * cols), coupling.dtype)
    right = kernel_call(right_kernel, facts, (coupling, part, rest), both)
    weighting = (own_weight, other_weight, right)

    summands = []
    for c in range(CHUNKS):
        held = [coupling[:, c * width : (c + 1) * width]]
        for step in range(1, 5):
            cores = (0, 1) if step < 4 else (late_core(c),)
            pairs = ring_pairs(Z, 1, cores)
            held.append(lax.ppermute(held[-1], ("f", "z"), pairs))
        base = FACTS + PER_CHUNK * c
        out = products(base + 2, facts, held, *weighting, jnp.bfloat16)
        near = products(base, facts, held, *weighting, jnp.float32)
        relay = lax.ppermute(out[0], ("f", "x"), ring_pairs(X, 1))
        back = lax.ppermute(out[1], ("f", "x"), ring_pairs(X, -1))
        ahead = (near[1] + relay.astype(jnp.float32)).astype(jnp.bfloat16)
        ahead = lax.ppermute(ahead, ("f", "x"), ring_pairs(X, 1))
        summands.append((near, back, ahead))

    pieces = []
    for group in GROUPS:
        count = len(group)
        both = (jax.ShapeDtypeStruct((count, width, YL * cols), jnp.float32),) * 2
        args = [part for c in group for part in summands[c]]
        mine, away = kernel_call(sum_kernel, facts, args, both)
        came = lax.ppermute(away, "f", SWAP)
        shapes = [jax.ShapeDtypeStruct((count * width, cols), jnp.float32)]
        shapes += [jax.ShapeDtypeStruct((count * width, cols), jnp.bfloat16)] * (YH * YL - 1)
        kernel = functools.partial(arrange_kernel, group)
        kept, *sent = kernel_call(kernel, facts, (mine, came), tuple(shapes))
        pieces.append(kept)
        for d in range(1, YH * YL):
            pairs = [(i, (i + d) % (YH * YL)) for i in range(YH * YL)]
            pieces.append(lax.ppermute(sent[d - 1], ("yh", "yl"), pairs))
    out = jax.ShapeDtypeStruct((YL * cols, cols), jnp.float32)
    return kernel_call(functools.partial(final_kernel, GROUPS), facts, pieces, out)


def solution(mesh):
    torus = Mesh(mesh.devices.reshape(FREQ, YH, X, Z, YL), AXES)
    placed = (P(("yh", "x"), ("z", "yl")), P(("f", "yh", "x")))

    return jax.shard_map(
        on_device,
        mesh=torus,
        in_specs=placed,
        out_specs=P(("f", "yh", "x"), ("z", "yl")),
        check_vma=False,
    )
```

```python
import functools

import jax
import jax.numpy as jnp
import numpy as np
from jax import lax
from jax.experimental import pallas as pl
from jax.experimental.pallas import tpu as pltpu
from jax.sharding import Mesh
from jax.sharding import PartitionSpec as P


FREQ, YH, X, Z, YL = 2, 2, 4, 8, 2
AXES = ("f", "yh", "x", "z", "yl")
CHUNKS = 3
GROUPS = ((0, 1), (2,))
SWAP = [(0, 1), (1, 0)]


FACTS, PER_CHUNK = 3, 5


def late_core(c):
    return 1 - c % 2


def lookup_table():
    rows = []
    for f, yh, x, z, yl in np.ndindex(FREQ, YH, X, Z, YL):
        row = [f, yh, yl]
        first = (z - x if f == 0 else x - z) % X
        for c in range(CHUNKS):
            at = [(first - delta) % X for delta in range(X)]
            at = [X if j == 0 and f == late_core(c) else j for j in at]
            home = ((z - at[0] if f == 0 else z + at[0]) % Z) // X
            row += at + [home]
        rows.append(row)
    return np.array(rows, np.int32)


def ring_pairs(size, sign, cores=(0, 1)):
    pairs = []
    for f in cores:
        step = sign if f == 0 else -sign
        pairs += [(f * size + i, f * size + (i + step) % size) for i in range(size)]
    return pairs


def kernel_call(kernel, facts, args, out_shape, flops=1 << 28, scratch_shapes=()):
    vmem = pl.BlockSpec(memory_space=pltpu.VMEM)
    return pl.pallas_call(
        kernel,
        out_shape=out_shape,
        in_specs=[pl.BlockSpec(memory_space=pltpu.SMEM)] + [vmem] * len(args),
        out_specs=jax.tree.map(lambda _: vmem, out_shape),
        scratch_shapes=scratch_shapes,
        compiler_params=pltpu.CompilerParams(vmem_limit_bytes=12 << 20),
        cost_estimate=pl.CostEstimate(flops=flops, bytes_accessed=4 << 20, transcendentals=0),
    )(facts, *args)


def copy_kernel(from_ref, to_ref):
    to_ref[...] = from_ref[...]


def cut(x, c, width):
    rows = x.shape[0]
    return pl.pallas_call(
        copy_kernel,
        grid=(1,),
        out_shape=jax.ShapeDtypeStruct((rows, width), x.dtype),
        in_specs=[pl.BlockSpec((rows, width), lambda i: (0, c))],
        out_specs=pl.BlockSpec(memory_space=pltpu.VMEM),
        compiler_params=pltpu.CompilerParams(vmem_limit_bytes=4 << 20),
    )(x)


def half_kernel(facts_ref, tile_ref, out_ref):
    rows = out_ref.shape[0]
    out_ref[...] = tile_ref[pl.ds(pl.multiple_of(facts_ref[0] * rows, rows), rows), :]


def right_kernel(facts_ref, own_ref, part_ref, rest_ref, out_ref):
    rows, cols = part_ref.shape
    for yl in range(YL):
        own_cols = slice(yl * cols, (yl + 1) * cols)
        other_cols = slice((1 - yl) * cols, (2 - yl) * cols)

        @pl.when(facts_ref[2] == yl)
        def _():
            out_ref[:, own_cols] = own_ref[...]
            for f in range(FREQ):
                mine, swapped = (pl.ds(h * rows, rows) for h in (f, 1 - f))

                @pl.when(facts_ref[0] == f)
                def _():
                    out_ref[mine, other_cols] = part_ref[...]
                    out_ref[swapped, other_cols] = rest_ref[...]


def product_kernel(base, facts_ref, *refs):
    tiles, (own_ref, other_ref, right_ref, out_ref, left_ref) = refs[:-5], refs[-5:]
    rows, width = tiles[0].shape
    tall = rows // 6 if rows % 96 == 0 else rows

    @pl.loop(0, out_ref.shape[0])
    def _(k):
        for number, tile_ref in enumerate(tiles):

            @pl.when(facts_ref[base + k] == number)
            def _():
                @pl.loop(0, rows // tall)
                def _(i):
                    part = pl.ds(i * tall, tall)
                    tile = tile_ref[part, :].astype(jnp.float32)
                    for g, weight_ref in enumerate((own_ref, other_ref)):
                        scaled = (tile * weight_ref[part, :]).astype(jnp.bfloat16)
                        left_ref[part, g * width : (g + 1) * width] = scaled

        out_ref[k] = lax.dot_general(
            left_ref[...],
            right_ref[...],
            (((0,), (0,)), ((), ())),
            preferred_element_type=jnp.float32,
        ).astype(out_ref.dtype)


def products(base, facts, tiles, own_weight, other_weight, right, dtype):
    rows, width = tiles[0].shape
    wide = right.shape[1]
    return kernel_call(
        functools.partial(product_kernel, base),
        facts,
        (*tiles, own_weight, other_weight, right),
        jax.ShapeDtypeStruct((2, FREQ * width, wide), dtype),
        4 * FREQ * width * wide * rows,
        (pltpu.VMEM((rows, FREQ * width), jnp.bfloat16),),
    )


def sum_kernel(facts_ref, *refs):
    parts, (mine_ref, away_ref) = refs[:-2], refs[-2:]
    width = mine_ref.shape[1]
    for i in range(mine_ref.shape[0]):
        own_ref, back_ref, ahead_ref = parts[3 * i : 3 * i + 3]
        for half, out_ref in enumerate((mine_ref, away_ref)):
            part = slice(half * width, (half + 1) * width)
            total = own_ref[0, part, :] + back_ref[part, :].astype(jnp.float32)
            total += ahead_ref[part, :].astype(jnp.float32)
            out_ref[i] = total.astype(out_ref.dtype)


def arrange_kernel(group, facts_ref, mine_ref, came_ref, kept_ref, *sent):
    width, cols = mine_ref.shape[1], mine_ref.shape[2] // YL
    here = facts_ref[1] * YL + facts_ref[2]
    for i, c in enumerate(group):
        part = pl.ds(i * width, width)
        home = facts_ref[FACTS + PER_CHUNK * c + X]
        for source_ref, away in ((mine_ref, 0), (came_ref, 1)):
            for there in range(YH * YL):
                yh, yl = divmod(there, YL)
                for d in range(YH * YL):

                    @pl.when((home == yh ^ away) & (here == (there - d) % (YH * YL)))
                    def _():
                        block = source_ref[i, :, yl * cols : (yl + 1) * cols]
                        out_ref = sent[d - 1] if d else kept_ref
                        out_ref[part, :] = block.astype(out_ref.dtype)


def final_kernel(groups, facts_ref, *refs):
    parts, (out_ref, done_ref, sem_ref) = refs[:-3], refs[-3:]
    cols = out_ref.shape[1]
    width = cols // CHUNKS
    copies = []
    for number, group in enumerate(groups):
        kept_ref, one_ref, two_ref, three_ref = parts[4 * number : 4 * number + 4]
        for i, c in enumerate(group):
            part = pl.ds(i * width, width)
            near = kept_ref[part, :] + two_ref[part, :].astype(jnp.float32)
            far = one_ref[part, :].astype(jnp.float32) + three_ref[part, :].astype(jnp.float32)
            for half, value in enumerate((near, far)):
                slot = 2 * c + half
                done_ref[slot] = value
                start = (facts_ref[2] ^ half) * cols + c * width
                start = pl.multiple_of(start, width)
                copies.append(
                    pltpu.make_async_copy(
                        done_ref.at[slot], out_ref.at[pl.ds(start, width), :], sem_ref.at[slot]
                    )
                )
                copies[-1].start()
    for copy in copies:
        copy.wait()


def write_sum(facts, pieces, cols):
    vmem = pl.BlockSpec(memory_space=pltpu.VMEM)
    return pl.pallas_call(
        functools.partial(final_kernel, GROUPS),
        out_shape=jax.ShapeDtypeStruct((YL * cols, cols), jnp.float32),
        in_specs=[pl.BlockSpec(memory_space=pltpu.SMEM)] + [vmem] * len(pieces),
        out_specs=pl.BlockSpec(memory_space=pl.ANY),
        scratch_shapes=[
            pltpu.VMEM((2 * CHUNKS, cols // CHUNKS, cols), jnp.float32),
            pltpu.SemaphoreType.DMA((2 * CHUNKS,)),
        ],
        compiler_params=pltpu.CompilerParams(vmem_limit_bytes=12 << 20),
    )(facts, *pieces)


def on_device(coupling, freq_weight):
    rows, cols = coupling.shape
    width = cols // CHUNKS
    facts = jnp.asarray(lookup_table())
    facts = lax.dynamic_index_in_dim(facts, lax.axis_index(AXES), keepdims=False)

    half = jax.ShapeDtypeStruct((rows // 2, cols), coupling.dtype)
    part = lax.ppermute(kernel_call(half_kernel, facts, (coupling,), half), "yl", SWAP)
    other_weight = lax.ppermute(freq_weight, "f", SWAP)
    own_weight, other_weight = (
        jnp.broadcast_to(w[:, None], (rows, width)) for w in (freq_weight, other_weight)
    )
    rest = lax.ppermute(part, "f", SWAP)
    both = jax.ShapeDtypeStruct((rows, YL * cols), coupling.dtype)
    right = kernel_call(right_kernel, facts, (coupling, part, rest), both)
    weighting = (own_weight, other_weight, right)

    summands = []
    for c in range(CHUNKS):
        held = [cut(coupling, c, width)]
        for step in range(1, 5):
            cores = (0, 1) if step < 4 else (late_core(c),)
            pairs = ring_pairs(Z, 1, cores)
            held.append(lax.ppermute(held[-1], ("f", "z"), pairs))
        base = FACTS + PER_CHUNK * c
        out = products(base + 2, facts, held, *weighting, jnp.bfloat16)
        near = products(base, facts, held, *weighting, jnp.float32)
        relay = lax.ppermute(out[0], ("f", "x"), ring_pairs(X, 1))
        back = lax.ppermute(out[1], ("f", "x"), ring_pairs(X, -1))
        ahead = (near[1] + relay.astype(jnp.float32)).astype(jnp.bfloat16)
        ahead = lax.ppermute(ahead, ("f", "x"), ring_pairs(X, 1))
        summands.append((near, back, ahead))

    pieces = []
    for group in GROUPS:
        count = len(group)
        both = tuple(
            jax.ShapeDtypeStruct((count, width, YL * cols), dtype)
            for dtype in (jnp.float32, jnp.bfloat16)
        )
        args = [part for c in group for part in summands[c]]
        mine, away = kernel_call(sum_kernel, facts, args, both)
        came = lax.ppermute(away, "f", SWAP)
        shapes = [jax.ShapeDtypeStruct((count * width, cols), jnp.float32)]
        shapes += [jax.ShapeDtypeStruct((count * width, cols), jnp.bfloat16)] * (YH * YL - 1)
        kernel = functools.partial(arrange_kernel, group)
        kept, *sent = kernel_call(kernel, facts, (mine, came), tuple(shapes))
        pieces.append(kept)
        for d in range(1, YH * YL):
            pairs = [(i, (i + d) % (YH * YL)) for i in range(YH * YL)]
            pieces.append(lax.ppermute(sent[d - 1], ("yh", "yl"), pairs))
    return write_sum(facts, pieces, cols)


def solution(mesh):
    torus = Mesh(mesh.devices.reshape(FREQ, YH, X, Z, YL), AXES)
    placed = (P(("yh", "x"), ("z", "yl")), P(("f", "yh", "x")))

    return jax.shard_map(
        on_device,
        mesh=torus,
        in_specs=placed,
        out_specs=P(("f", "yh", "x"), ("z", "yl")),
        check_vma=False,
    )
```
